32 devices in a mesh: groups: 2 (over y), seq: 4 (over z), head: 4 (over x, core).
Axes of the slice: x: 2, y: 2, z: 4, core: 2. Of those that a mesh axis runs over, the one named last changes fastest.
Arguments:
- query: bfloat16 [4, 8192], P('groups', 'head'), parts along dimension 0, may hold values from -170 to 170
- cache_keys: bfloat16 [4, 1024, 1024], P('groups', 'seq', 'head'), parts along dimension 0, may hold values from -6 to 6
- cache_values: bfloat16 [4, 1024, 1024], P('groups', 'seq', 'head'), parts along dimension 0, may hold values from -6 to 6
- lengths: int32 [4], P('groups'), parts along dimension 0, may hold values from 256 to 1024
- heavy: int32 [4, 2], P('groups'), parts along dimension 0, may hold values from 0 to 7, as said below
- acc_scores: float32 [4, 8], P('groups', 'seq'), parts along dimension 0, may hold values from 0.01 to 1
- refill_kv: bfloat16 [64, 2, 128, 128], P(('groups', 'seq', 'head')), parts along dimension 0, may hold values from -6 to 6
- refill_dest: int32 [64, 1], P(('groups', 'seq', 'head')), parts along dimension 0, may hold values from 0 to 3, as said below
- refill_req: int32 [64], P(('groups', 'seq', 'head')), parts along dimension 0, may hold values from 0 to 1
- refill_head: int32 [64], P(('groups', 'seq', 'head')), parts along dimension 0, may hold values from 0 to 1
Outputs:
- attn_out: bfloat16 [4, 8192], P('groups'), parts along dimension 0
- block_scores: float32 [4, 8], P('groups', 'seq'), parts along dimension 0
- recalled_kv: bfloat16 [64, 2, 128, 128], P(('groups', 'seq', 'head')), parts along dimension 0
- recall_scores: float32 [32, 2], P(('groups', 'seq', 'head')), parts along dimension 0
The draws below stay inside these ranges and needn't reach their ends.
There are 2 independent parts, one for each index of `groups`. The reference program is written for one: setup_inputs(seed, part) draws one part's arguments, and reference() takes and returns one part's arrays. A program takes and returns all parts, laid end to end along the dimension named above; each array names one. Nothing has to cross between parts.
Inputs may be any that keep to these rules, and one draw needn't show every extreme that they name: `heavy`: the 2 block ids of one request are distinct. `refill_dest`: the block at position j of device (s, h) goes to owner (s + k) mod 4, with k fixed by h and j alone; among the 2 blocks of one device at most 2 name the same owner, and on every device 2 do.
All inputs are finite; a program needn't handle non-finite values.
Results may differ from the reference program's by a relative error of at most 0.0045.
Values may be sent and summed in bfloat16 or wider, within the bound.
No kernel may reach another device: no remote copies, remote signals or barrier semaphores. Data moves between devices by JAX's collectives and lax.ppermute only.
A program may use at most 128 MiB of HBM per device.

```python
import math
import jax
import jax.numpy as jnp
from jax import lax

HQ = 64
KVH = 8
DH = 128
BLKTOK = 128
RECENT = 2
BATCH = 2
NBLK = 8
SEQLEN = 1024
NHEAVY = 2
REFILL_DEV = 2
UNITS = 32
N_SEQ = 4
N_HEAD = 4


def lengths_helper(subkey):
    drawn = jax.random.randint(jax.random.fold_in(subkey, 1), (BATCH,), SEQLEN // 4, SEQLEN + 1).astype(jnp.int32)
    fullest = jax.random.randint(jax.random.fold_in(subkey, 2), (), 0, BATCH).astype(jnp.int32)
    return jnp.where(jnp.arange(BATCH, dtype=jnp.int32) == fullest, SEQLEN, drawn).astype(jnp.int32)


def keys_helper(basekey):
    base = jnp.clip(jax.random.normal(jax.random.fold_in(basekey, 12), (BATCH, SEQLEN, KVH * DH), jnp.float32), -6.0, 6.0)
    return base


def draw_lengths(key, part):
    return lengths_helper(jax.random.fold_in(key, 11))


def draw_cache_keys(key, part):
    return keys_helper(key).astype(jnp.bfloat16)


def draw_query(key, part):
    base = jnp.clip(jax.random.normal(jax.random.fold_in(key, 21), (BATCH, HQ, DH), jnp.float32), -6.0, 6.0)
    head_frac = jnp.arange(HQ, dtype=jnp.float32) / (HQ - 1)
    rising = jnp.power(4.0, head_frac)
    base = base * rising[None, :, None]
    return base.reshape(BATCH, HQ * DH).astype(jnp.bfloat16)


def pick_blocks(subkey):
    return jax.random.permutation(subkey, NBLK)[:NHEAVY]


def draw_heavy(key, part):
    subkeys = jax.random.split(jax.random.fold_in(key, 31), BATCH)
    return jax.vmap(pick_blocks)(subkeys).astype(jnp.int32)


def pick_steps(subkey):
    order = jax.random.permutation(subkey, N_SEQ)[:REFILL_DEV]
    return order.at[1].set(order[0])


def draw_refill_dest(key, part):
    subkeys = jax.random.split(jax.random.fold_in(key, 41), N_HEAD)
    steps_table = jax.vmap(pick_steps)(subkeys).astype(jnp.int32)
    unit_ids = jnp.arange(UNITS, dtype=jnp.int32)
    source = unit_ids // REFILL_DEV
    place = unit_ids % REFILL_DEV
    head_dev = source % N_HEAD
    seq_src = source // N_HEAD
    owner = (seq_src + steps_table[head_dev, place]) % N_SEQ
    return owner.astype(jnp.int32).reshape(UNITS, 1)


def place_ends(array, stream_key, smallest, top_value):
    index_at = [jax.random.randint(jax.random.fold_in(stream_key, axis), (), 0, length) for axis, length in enumerate(array.shape)]
    widest = array.shape.index(max(array.shape))
    next_to = index_at[:widest] + [(index_at[widest] + 1) % array.shape[widest]] + index_at[widest + 1:]
    return array.at[tuple(index_at)].set(smallest).at[tuple(next_to)].set(top_value)


def levels(stream_key, extent, pieces, smallest, high):
    loudness, own = 1.0, jax.random.fold_in(stream_key, 6)
    for dim, shards_of in pieces:
        heights = jnp.exp(jax.random.uniform(jax.random.fold_in(own, dim), (shards_of,), jnp.float32, smallest / len(pieces), high / len(pieces)))
        loudness = loudness * jnp.repeat(heights, extent[dim] // shards_of).reshape([-1 if axis == dim else 1 for axis in range(len(extent))])
    return loudness


def scatter_about(rng, dims, scale, reach, cuts=(), held_as=jnp.bfloat16):
    array = jax.random.normal(rng, dims, jnp.float32) * scale
    if len(cuts) > 0:
        array = levels(rng, dims, cuts, -0.22, 0.18) * array
    return jnp.clip(array, min=-reach, max=reach).astype(held_as)


def setup_inputs(seed: int = 0, part: int = 0) -> dict:
    key_of = jax.random.split(jax.random.key(seed), 11)
    part_keys = jax.random.split(jax.random.fold_in(key_of[10], part), 11)
    query = draw_query(jax.random.fold_in(jax.random.fold_in(key_of[10], part), 71), part)
    cache_keys = draw_cache_keys(jax.random.fold_in(jax.random.fold_in(key_of[10], part), 71), part)
    cache_values = scatter_about(part_keys[2], (BATCH, SEQLEN, KVH * DH), 1.0, 6.0, ((1, 4), (2, 4)))
    lengths = draw_lengths(jax.random.fold_in(jax.random.fold_in(key_of[10], part), 71), part)
    heavy = draw_heavy(jax.random.fold_in(jax.random.fold_in(key_of[10], part), 71), part)
    acc_scores = jnp.clip(jnp.exp(math.log(1.0) - 4.6051702 * jax.random.uniform(part_keys[5], (BATCH, NBLK), jnp.float32) ** levels(part_keys[5], (BATCH, NBLK), ((1, 4),), -0.2, 0.2)), 0.01, 1.0)
    refill_kv = scatter_about(part_keys[6], (UNITS, 2, BLKTOK, DH), 1.0, 6.0, ((0, 16),))
    refill_dest = draw_refill_dest(jax.random.fold_in(jax.random.fold_in(key_of[10], part), 71), part)
    refill_req = place_ends(jax.random.randint(part_keys[8], (UNITS,), 0, BATCH), jax.random.fold_in(part_keys[8], 1), 0, BATCH - 1).astype(jnp.int32)
    refill_head = place_ends(jax.random.randint(part_keys[9], (UNITS,), 0, KVH // N_HEAD), jax.random.fold_in(part_keys[9], 1), 0, (KVH // N_HEAD) - 1).astype(jnp.int32)
    return {"query": query, "cache_keys": cache_keys, "cache_values": cache_values, "lengths": lengths, "heavy": heavy, "acc_scores": acc_scores, "refill_kv": refill_kv, "refill_dest": refill_dest, "refill_req": refill_req, "refill_head": refill_head}


def reference(query, cache_keys, cache_values, lengths, heavy, acc_scores, refill_kv, refill_dest, refill_req, refill_head):
    per_group = HQ // KVH
    kv_local = KVH // N_HEAD
    score_scale = 1.0 / math.sqrt(DH)
    hiprec = lax.Precision.HIGHEST
    q_four = query.astype(jnp.float32).reshape(BATCH, KVH, per_group, DH)
    position = jnp.arange(SEQLEN, dtype=jnp.int32)
    block_ids = jnp.arange(NBLK, dtype=jnp.int32)
    heavy_hit = jnp.any(heavy[:, :, None] == block_ids[None, None, :], axis=1)
    recent = block_ids[None, :] >= ((lengths - 1) // BLKTOK - (RECENT - 1))[:, None]
    kept = jnp.repeat(heavy_hit | recent, BLKTOK, axis=1) & (position[None, :] < lengths[:, None])
    keys_four = cache_keys.astype(jnp.float32).reshape(BATCH, SEQLEN, KVH, DH)
    values_four = cache_values.astype(jnp.float32).reshape(BATCH, SEQLEN, KVH, DH)
    scores = jnp.einsum('bkgd,btkd->bkgt', q_four, keys_four, precision=hiprec) * score_scale
    masked = jnp.where(kept[:, None, None, :], scores, -1e+30)
    unit_ids = jnp.arange(UNITS, dtype=jnp.int32)
    source = unit_ids // REFILL_DEV
    place = unit_ids % REFILL_DEV
    head_dev = source % N_HEAD
    unit_kvh = head_dev * kv_local + refill_head
    segment = refill_req * KVH + unit_kvh
    q_units = q_four.reshape(BATCH * KVH, per_group, DH)[segment]
    unit_keys = refill_kv[:, 0].astype(jnp.float32)
    unit_vals = refill_kv[:, 1].astype(jnp.float32)
    unit_scores = jnp.einsum('ugd,urd->ugr', q_units, unit_keys, precision=hiprec) * score_scale
    seg_top = jnp.full((BATCH * KVH, per_group), -1e+30, jnp.float32).at[segment].max(lax.optimization_barrier(jnp.max(unit_scores, axis=2)))
    cache_top = lax.optimization_barrier(jnp.max(masked, axis=3)).reshape(BATCH * KVH, per_group)
    row_top = jnp.maximum(cache_top, seg_top)
    top_four = row_top.reshape(BATCH, KVH, per_group, 1)
    cache_exp = jnp.where(kept[:, None, None, :], jnp.exp(masked - top_four), 0.0)
    unit_exp = jnp.exp(unit_scores - row_top[segment][:, :, None])
    total = lax.optimization_barrier(jnp.sum(cache_exp, axis=3)).reshape(BATCH * KVH, per_group)
    total = total + jax.ops.segment_sum(lax.optimization_barrier(jnp.sum(unit_exp, axis=2)), segment, num_segments=BATCH * KVH)
    cache_wts = lax.optimization_barrier(cache_exp.astype(jnp.bfloat16)).astype(jnp.float32)
    unit_wts = lax.optimization_barrier(unit_exp.astype(jnp.bfloat16)).astype(jnp.float32)
    accum = jnp.einsum('bkgt,btkd->bkgd', cache_wts, values_four, precision=hiprec).reshape(BATCH * KVH, per_group, DH)
    unit_pv = jnp.einsum('ugr,urd->ugd', unit_wts, unit_vals, precision=hiprec)
    accum = accum + jax.ops.segment_sum(unit_pv, segment, num_segments=BATCH * KVH)
    attn_out = (accum / total[:, :, None]).astype(jnp.bfloat16).reshape(BATCH, HQ * DH)
    total_four = total.reshape(BATCH, KVH, per_group, 1)
    token_mass = lax.optimization_barrier(jnp.sum(cache_exp / total_four, axis=(1, 2)))
    block_scores = acc_scores + token_mass.reshape(BATCH, NBLK, BLKTOK).sum(axis=2)
    unit_mass = lax.optimization_barrier(jnp.sum(unit_exp / total[segment][:, :, None], axis=(1, 2)))
    rows_out = refill_dest[:, 0] * N_HEAD + head_dev
    target = rows_out * REFILL_DEV + place
    recalled_kv = jnp.zeros_like(refill_kv).at[target].set(refill_kv)
    recall_scores = jnp.zeros((N_SEQ * N_HEAD, REFILL_DEV), jnp.float32).at[rows_out, place].set(unit_mass)
    return (attn_out, block_scores, recalled_kv, recall_scores)
```

```python
import functools
import math

import jax
import jax.numpy as jnp
from jax import lax
from jax.experimental import pallas as pl
from jax.experimental.pallas import tpu as pltpu
from jax.sharding import PartitionSpec as P

DH = 128
BLKTOK = 128
RECENT = 2
CAP = 2
LANES = 128
FEW = 8

NEG_BIG = -1e30


def round_up(value, step):
    return (value + step - 1) // step * step


def by_flips(count):
    return 1 < count <= FEW and count & (count - 1) == 0


def flip(value, axis, mask):
    count = lax.axis_size(axis)
    return lax.ppermute(value, axis, [(at, at ^ mask) for at in range(count)])


def exchange(value, axis):
    count = lax.axis_size(axis)
    if by_flips(count):
        return (value,) + tuple(flip(value, axis, mask) for mask in range(1, count))
    return (lax.all_gather(value, axis),)


def pieces_of(refs, count):
    if len(refs) == count:
        return [ref[...] for ref in refs]
    return [refs[0][at] for at in range(count)]


def source_of(index, count, flips, at):
    return index ^ at if flips else jnp.int32(at)


def tree_sum(values):
    values = list(values)
    while len(values) > 1:
        pairs = [values[at] + values[at + 1] for at in range(0, len(values) - 1, 2)]
        if len(values) % 2:
            pairs.append(values[-1])
        values = pairs
    return values[0]


def nt_dot(left, right):
    return lax.dot_general(
        left, right, (((1,), (1,)), ((), ())), preferred_element_type=jnp.float32
    )


def nn_dot(left, right):
    return lax.dot_general(
        left, right, (((1,), (0,)), ((), ())), preferred_element_type=jnp.float32
    )


def local_kernel(
    lengths_hbm,
    heavy_hbm,
    req_hbm,
    head_hbm,
    query_hbm,
    keys_hbm,
    values_hbm,
    refill_hbm,
    part_ref,
    block_ref,
    lengths,
    heavy,
    req,
    unit_head,
    query,
    keys,
    values,
    refill,
    sems,
):
    pairs = (
        (lengths_hbm, lengths),
        (heavy_hbm, heavy),
        (req_hbm, req),
        (head_hbm, unit_head),
        (query_hbm, query),
        (keys_hbm, keys),
        (refill_hbm, refill),
        (values_hbm, values),
    )
    copies = [pltpu.make_async_copy(src, dst, sems.at[at]) for at, (src, dst) in enumerate(pairs)]
    for copy in copies:
        copy.start()
    requests, width = query.shape
    heads_local = width // DH
    seq_local = keys.shape[1]
    kv_local = keys.shape[2] // DH
    per_group = heads_local // kv_local
    held = refill.shape[0]
    nheavy = heavy.shape[1]
    blocks_local = seq_local // BLKTOK
    rows = heads_local * requests
    group_rows = per_group * requests
    score_scale = 1.0 / math.sqrt(DH)
    seq_index = lax.axis_index("seq")

    row = lax.broadcasted_iota(jnp.int32, (rows, 1), 0)
    row_req = lax.rem(row, requests)
    row_group = lax.div(row, group_rows)
    lane = lax.broadcasted_iota(jnp.int32, (1, seq_local), 1)
    position = lane + seq_index * seq_local
    lane_block = lax.div(lane, BLKTOK)
    for copy in copies[:4]:
        copy.wait()
    kept = None
    for b in range(requests):
        length = lengths[b]
        first_recent = lax.div(length - 1, BLKTOK) - (RECENT - 1)
        open_block = jnp.zeros((1, seq_local), jnp.int32)
        for j in range(blocks_local):
            block_id = seq_index * blocks_local + j
            hit = block_id >= first_recent
            for t in range(nheavy):
                hit = hit | (heavy[b, t] == block_id)
            open_block = jnp.where(lane_block == j, hit.astype(jnp.int32), open_block)
        kept_b = jnp.where(position < length, open_block, 0)
        kept_b = jnp.broadcast_to(kept_b, (rows, seq_local))
        kept = kept_b if kept is None else jnp.where(row_req == b, kept_b, kept)
    kept = kept > 0

    copies[4].wait()
    q_wide = query[...].astype(jnp.float32)
    q_rows = jnp.concatenate(
        [q_wide[:, i * DH : (i + 1) * DH] for i in range(heads_local)], axis=0
    ).astype(jnp.bfloat16)
    copies[5].wait()
    scores = []
    for g in range(kv_local):
        q_group = q_rows[g * group_rows : (g + 1) * group_rows]
        req_group = row_req[g * group_rows : (g + 1) * group_rows]
        found = None
        for b in range(requests):
            dots = nt_dot(q_group, keys[b, :, g * DH : (g + 1) * DH])
            found = dots if found is None else jnp.where(req_group == b, dots, found)
        scores.append(found)
    scores = jnp.concatenate(scores, axis=0) * score_scale
    masked = jnp.where(kept, scores, NEG_BIG)
    best = jnp.max(masked, axis=1, keepdims=True)

    copies[6].wait()
    unit_masked, unit_on = [], []
    for u in range(held):
        on = (row_group == unit_head[u]) & (row_req == req[u])
        dots = nt_dot(q_rows, refill[u, 0]) * score_scale
        dots = jnp.where(on, dots, NEG_BIG)
        unit_masked.append(dots)
        unit_on.append(on)
        best = jnp.maximum(best, jnp.max(dots, axis=1, keepdims=True))

    stat_lane = lax.broadcasted_iota(jnp.int32, (rows, LANES), 1)
    probs = jnp.where(kept, jnp.exp(masked - best), 0.0)
    total = jnp.sum(probs, axis=1, keepdims=True)
    block_cols = jnp.zeros((rows, LANES), jnp.float32)
    for j in range(blocks_local):
        mass = jnp.sum(probs[:, j * BLKTOK : (j + 1) * BLKTOK], axis=1, keepdims=True)
        block_cols = jnp.where(lax.rem(stat_lane, blocks_local) == j, mass, block_cols)
    block_ref[...] = block_cols
    stats = jnp.where(stat_lane == 0, best, 0.0)
    unit_probs = []
    for u in range(held):
        weight = jnp.where(unit_on[u], jnp.exp(unit_masked[u] - best), 0.0)
        mass = jnp.sum(weight, axis=1, keepdims=True)
        total = total + mass
        stats = jnp.where(stat_lane == 2 + u, mass, stats)
        unit_probs.append(weight.astype(jnp.bfloat16))
    stats = jnp.where(stat_lane == 1, total, stats)

    copies[7].wait()
    accum = []
    for g in range(kv_local):
        probs_group = probs[g * group_rows : (g + 1) * group_rows]
        req_group = row_req[g * group_rows : (g + 1) * group_rows]
        accum.append(
            tree_sum(
                nn_dot(
                    jnp.where(req_group == b, probs_group, 0.0).astype(jnp.bfloat16),
                    values[b, :, g * DH : (g + 1) * DH],
                )
                for b in range(requests)
            )
        )
    accum = jnp.concatenate(accum, axis=0)
    for u in range(held):
        accum = accum + nn_dot(unit_probs[u], refill[u, 1])
    part_ref[:rows, :] = accum
    stat_rows = part_ref.shape[0] - rows
    turned = jnp.transpose(stats)
    part_ref[rows:, :] = jnp.zeros((stat_rows, LANES), jnp.float32)
    part_ref[rows:, :rows] = turned[:stat_rows]


def middle_kernel(flips, count, rows, requests, blocks_local, dest, *refs):
    part_refs = refs[:-3]
    block_ref, head_ref, recall_ref = refs[-3:]
    held = dest.shape[0]
    seq_index = lax.axis_index("seq")
    pieces = pieces_of(part_refs, count)
    stat_rows = pieces[0].shape[0] - rows
    turned = jnp.transpose(jnp.concatenate([piece[rows:] for piece in pieces], axis=0))
    stats = [turned[:rows, at * stat_rows : (at + 1) * stat_rows] for at in range(count)]
    best = functools.reduce(jnp.maximum, [stat[:, 0:1] for stat in stats])
    factors = [jnp.exp(stat[:, 0:1] - best) for stat in stats]
    total = tree_sum(stat[:, 1:2] * factor for stat, factor in zip(stats, factors))
    accum = tree_sum(piece[:rows] * factor for piece, factor in zip(pieces, factors))
    head_ref[:rows, :] = (accum / total).astype(jnp.bfloat16)

    lane = lax.broadcasted_iota(jnp.int32, (1, held), 1)
    origin = jnp.zeros((1, held), jnp.int32)
    for j in range(held):
        steps = lax.rem(dest[j, 0] - seq_index + count, count)
        origin = jnp.where(lane == j, lax.rem(seq_index - steps + count, count), origin)
    recall = jnp.zeros((1, held), jnp.float32)
    for at in range(count):
        share = stats[at][:, 2 : 2 + held] * factors[at] / total
        mass = jnp.sum(share, axis=0, keepdims=True)
        recall = jnp.where(origin == source_of(seq_index, count, flips, at), mass, recall)
    recall_ref[...] = recall

    if flips:
        own = factors[0]
    else:
        own = functools.reduce(
            lambda found, at: jnp.where(seq_index == at, factors[at], found),
            range(1, count),
            factors[0],
        )
    row = lax.broadcasted_iota(jnp.int32, (rows, LANES), 0)
    lanes = lax.broadcasted_iota(jnp.int32, (rows, LANES), 1)
    mine = lax.rem(row, requests) == lax.div(lanes, blocks_local)
    mass = jnp.sum(jnp.where(mine, block_ref[...] * own / total, 0.0), axis=0, keepdims=True)
    high = mass.astype(jnp.bfloat16).astype(jnp.float32)
    middle = (mass - high).astype(jnp.bfloat16).astype(jnp.float32)
    low = mass - high - middle
    extra = head_ref.shape[0] - rows
    line = lax.broadcasted_iota(jnp.int32, (extra, LANES), 0)
    packed = jnp.where(line == 0, high, jnp.where(line == 1, middle, 0.0))
    packed = jnp.where(line == 2, low, packed)
    head_ref[rows:, :] = packed.astype(jnp.bfloat16)


def final_kernel(flips, count, rows, requests, acc_ref, *refs):
    piece_refs = refs[:-2]
    out_ref, block_ref = refs[-2:]
    head_index = lax.axis_index("head")
    blocks_local = acc_ref.shape[1]
    pieces = pieces_of(piece_refs, count)
    for at, piece in enumerate(pieces):
        start = source_of(head_index, count, flips, at) * rows
        out_ref[pl.ds(pl.multiple_of(start, rows), rows), :] = piece[:rows]
    masses = []
    for piece in pieces:
        lines = piece[rows:].astype(jnp.float32)
        masses.append(lines[0:1] + lines[1:2] + lines[2:3])
    mass = tree_sum(masses)
    lanes = lax.broadcasted_iota(jnp.int32, (1, LANES), 1)
    at_req = lax.broadcasted_iota(jnp.int32, (requests, blocks_local), 0)
    at_block = lax.broadcasted_iota(jnp.int32, (requests, blocks_local), 1)
    added = acc_ref[...]
    for b in range(requests):
        for j in range(blocks_local):
            one = jnp.sum(jnp.where(lanes == b * blocks_local + j, mass, 0.0), axis=1, keepdims=True)
            added = jnp.where((at_req == b) & (at_block == j), added + one, added)
    block_ref[...] = added


def move_blocks(refill_kv, owners, seq_index, seq_count):
    held = refill_kv.shape[0]
    steps = (owners - seq_index) % seq_count
    if held == CAP and seq_count == 1 << CAP:
        step = steps[0]
        high, low = seq_count // 2, 1
        across = flip(refill_kv, "seq", high)
        wanted = ((seq_index ^ low) - step) % seq_count
        passed = jnp.where(wanted == seq_index, refill_kv, across)
        beside = flip(passed, "seq", low)
        source = (seq_index - step) % seq_count
        return jnp.where(
            source == seq_index,
            refill_kv,
            jnp.where(source == seq_index ^ high, across, beside),
        )
    earlier = jnp.arange(held)[:, None] > jnp.arange(held)[None, :]
    order_in = jnp.sum((owners[:, None] == owners[None, :]) & earlier, axis=1)
    slots = seq_count * CAP
    slot_of = owners * CAP + order_in
    pick = (seq_index - steps) % seq_count * CAP + order_in
    buffer = jnp.zeros((slots,) + refill_kv.shape[1:], refill_kv.dtype).at[slot_of].set(refill_kv)
    got = lax.all_to_all(
        buffer.reshape((seq_count, CAP) + refill_kv.shape[1:]),
        "seq",
        split_axis=0,
        concat_axis=0,
        tiled=True,
    )
    return got.reshape((slots,) + refill_kv.shape[1:])[pick]


def on_device(
    query,
    cache_keys,
    cache_values,
    lengths,
    heavy,
    acc_scores,
    refill_kv,
    refill_dest,
    refill_req,
    refill_head,
):
    requests, width = query.shape
    heads_local = width // DH
    rows = heads_local * requests
    held = refill_kv.shape[0]
    blocks_local = cache_keys.shape[1] // BLKTOK
    seq_count = lax.axis_size("seq")
    head_count = lax.axis_size("head")
    seq_index = lax.axis_index("seq")
    hbm = pl.BlockSpec(memory_space=pl.ANY)
    vmem = pl.BlockSpec(memory_space=pltpu.VMEM)
    smem = pl.BlockSpec(memory_space=pltpu.SMEM)
    stat_rows = round_up(2 + held, 8)
    inputs = (lengths, heavy, refill_req, refill_head, query, cache_keys, cache_values, refill_kv)

    recalled_kv = move_blocks(refill_kv, refill_dest[:, 0], seq_index, seq_count)

    part, block_part = pl.pallas_call(
        local_kernel,
        out_shape=(
            jax.ShapeDtypeStruct((rows + stat_rows, LANES), jnp.float32),
            jax.ShapeDtypeStruct((rows, LANES), jnp.float32),
        ),
        in_specs=[hbm] * len(inputs),
        out_specs=(vmem, vmem),
        scratch_shapes=[pltpu.SMEM(value.shape, value.dtype) for value in inputs[:4]]
        + [pltpu.VMEM(value.shape, value.dtype) for value in inputs[4:]]
        + [pltpu.SemaphoreType.DMA((len(inputs),))],
        name="local_attention",
    )(*inputs)

    parts = exchange(part, "seq")
    head_part, recall_scores = pl.pallas_call(
        functools.partial(
            middle_kernel, by_flips(seq_count), seq_count, rows, requests, blocks_local
        ),
        out_shape=(
            jax.ShapeDtypeStruct((rows + 16, LANES), jnp.bfloat16),
            jax.ShapeDtypeStruct((1, held), jnp.float32),
        ),
        in_specs=[smem] + [vmem] * (len(parts) + 1),
        out_specs=(vmem, vmem),
        name="combine_seq",
    )(refill_dest, *parts, block_part)

    head_parts = exchange(head_part, "head")
    attn_rows, block_scores = pl.pallas_call(
        functools.partial(final_kernel, by_flips(head_count), head_count, rows, requests),
        out_shape=(
            jax.ShapeDtypeStruct((head_count * rows, LANES), jnp.bfloat16),
            jax.ShapeDtypeStruct(acc_scores.shape, jnp.float32),
        ),
        in_specs=[vmem] * (len(head_parts) + 1),
        out_specs=(vmem, vmem),
        name="join_heads",
    )(acc_scores, *head_parts)
    attn_out = (
        attn_rows.reshape(head_count * heads_local, requests, DH)
        .transpose(1, 0, 2)
        .reshape(requests, head_count * width)
    )
    return (attn_out, block_scores, recalled_kv, recall_scores)


def solution(mesh):
    in_specs = (
        P("groups", "head"),
        P("groups", "seq", "head"),
        P("groups", "seq", "head"),
        P("groups"),
        P("groups", None),
        P("groups", "seq"),
        P(("groups", "seq", "head"), None, None, None),
        P(("groups", "seq", "head"), None),
        P(("groups", "seq", "head")),
        P(("groups", "seq", "head")),
    )
    out_specs = (
        P("groups", None),
        P("groups", "seq"),
        P(("groups", "seq", "head"), None, None, None),
        P(("groups", "seq", "head"), None),
    )
    return jax.shard_map(
        on_device, mesh=mesh, in_specs=in_specs, out_specs=out_specs, check_vma=False
    )
```

```python
import functools
import math

import jax
import jax.numpy as jnp
from jax import lax
from jax.experimental import pallas as pl
from jax.experimental.pallas import tpu as pltpu
from jax.sharding import PartitionSpec as P


DH = 128
BLKTOK = 128
RECENT = 2
CAP = 2
LANES = 128
FEW = 8

NEG_BIG = -1e30


def round_up(value, step):
    return (value + step - 1) // step * step


def by_flips(count):
    return 1 < count <= FEW and count & (count - 1) == 0


def flip(value, axis, mask):
    count = lax.axis_size(axis)
    return lax.ppermute(value, axis, [(at, at ^ mask) for at in range(count)])


def exchange(value, axis):
    count = lax.axis_size(axis)
    if by_flips(count):
        return (value,) + tuple(flip(value, axis, mask) for mask in range(1, count))
    return (lax.all_gather(value, axis),)


def near(value):
    return pltpu.with_memory_space_constraint(value, pltpu.VMEM)


def pieces_of(refs, count):
    if len(refs) == count:
        return [ref[...] for ref in refs]
    return [refs[0][at] for at in range(count)]


def source_of(index, flips, at):
    return index ^ at if flips else jnp.int32(at)


def tree_sum(values):
    values = list(values)
    while len(values) > 1:
        pairs = [values[at] + values[at + 1] for at in range(0, len(values) - 1, 2)]
        if len(values) % 2:
            pairs.append(values[-1])
        values = pairs
    return values[0]


def nt_dot(left, right):
    return lax.dot_general(
        left, right, (((1,), (1,)), ((), ())), preferred_element_type=jnp.float32
    )


def nn_dot(left, right):
    return lax.dot_general(
        left, right, (((1,), (0,)), ((), ())), preferred_element_type=jnp.float32
    )


def local_kernel(
    lengths_hbm,
    heavy_hbm,
    req_hbm,
    head_hbm,
    dest_hbm,
    query_hbm,
    keys_hbm,
    values_hbm,
    refill_hbm,
    part_ref,
    block_ref,
    route_ref,
    refill,
    lengths,
    heavy,
    req,
    unit_head,
    dest,
    query,
    keys,
    values,
    sems,
):
    pairs = (
        (lengths_hbm, lengths),
        (heavy_hbm, heavy),
        (req_hbm, req),
        (head_hbm, unit_head),
        (dest_hbm, dest),
        (query_hbm, query),
        (keys_hbm, keys),
        (refill_hbm, refill),
        (values_hbm, values),
    )
    copies = [pltpu.make_async_copy(src, dst, sems.at[at]) for at, (src, dst) in enumerate(pairs)]
    for copy in copies:
        copy.start()
    requests, width = query.shape
    heads_local = width // DH
    seq_local = keys.shape[1]
    kv_local = keys.shape[2] // DH
    per_group = heads_local // kv_local
    held = refill.shape[0]
    nheavy = heavy.shape[1]
    blocks_local = seq_local // BLKTOK
    rows = heads_local * requests
    group_rows = per_group * requests
    score_scale = 1.0 / math.sqrt(DH)
    seq_index = lax.axis_index("seq")

    row = lax.broadcasted_iota(jnp.int32, (rows, 1), 0)
    row_req = lax.rem(row, requests)
    row_group = lax.div(row, group_rows)
    lane = lax.broadcasted_iota(jnp.int32, (1, seq_local), 1)
    position = lane + seq_index * seq_local
    lane_block = lax.div(lane, BLKTOK)
    for copy in copies[:5]:
        copy.wait()
    seq_count = lax.axis_size("seq")
    origin = jnp.zeros((1, LANES), jnp.int32)
    route_lane = lax.broadcasted_iota(jnp.int32, (1, LANES), 1)
    for u in range(held):
        steps = lax.rem(dest[u] - seq_index + seq_count, seq_count)
        origin = jnp.where(
            route_lane == u, lax.rem(seq_index - steps + seq_count, seq_count), origin
        )
    steps = lax.rem(dest[0] - seq_index + seq_count, seq_count)
    source = lax.rem(seq_index - steps + seq_count, seq_count)
    wanted = lax.rem((seq_index ^ 1) - steps + seq_count, seq_count)
    route_row = lax.broadcasted_iota(jnp.int32, (8, LANES), 0)
    route = jnp.broadcast_to(origin, (8, LANES))
    route = jnp.where(route_row == 1, (wanted == seq_index).astype(jnp.int32), route)
    route = jnp.where(route_row == 2, (source == seq_index).astype(jnp.int32), route)
    far = seq_index ^ (seq_count // 2)
    route_ref[...] = jnp.where(route_row == 3, (source == far).astype(jnp.int32), route)
    kept = None
    for b in range(requests):
        length = lengths[b]
        first_recent = lax.div(length - 1, BLKTOK) - (RECENT - 1)
        open_block = jnp.zeros((1, seq_local), jnp.int32)
        for j in range(blocks_local):
            block_id = seq_index * blocks_local + j
            hit = block_id >= first_recent
            for t in range(nheavy):
                hit = hit | (heavy[b, t] == block_id)
            open_block = jnp.where(lane_block == j, hit.astype(jnp.int32), open_block)
        kept_b = jnp.where(position < length, open_block, 0)
        kept_b = jnp.broadcast_to(kept_b, (rows, seq_local))
        kept = kept_b if kept is None else jnp.where(row_req == b, kept_b, kept)
    kept = kept > 0

    copies[5].wait()
    q_wide = query[...].astype(jnp.float32)
    q_rows = jnp.concatenate(
        [q_wide[:, i * DH : (i + 1) * DH] for i in range(heads_local)], axis=0
    ).astype(jnp.bfloat16)
    copies[6].wait()
    scores = []
    for g in range(kv_local):
        q_group = q_rows[g * group_rows : (g + 1) * group_rows]
        req_group = row_req[g * group_rows : (g + 1) * group_rows]
        found = None
        for b in range(requests):
            dots = nt_dot(q_group, keys[b, :, g * DH : (g + 1) * DH])
            found = dots if found is None else jnp.where(req_group == b, dots, found)
        scores.append(found)
    scores = jnp.concatenate(scores, axis=0) * score_scale
    masked = jnp.where(kept, scores, NEG_BIG)
    best = jnp.max(masked, axis=1, keepdims=True)

    copies[7].wait()
    unit_masked, unit_on = [], []
    for u in range(held):
        on = (row_group == unit_head[u]) & (row_req == req[u])
        dots = nt_dot(q_rows, refill[u, 0]) * score_scale
        dots = jnp.where(on, dots, NEG_BIG)
        unit_masked.append(dots)
        unit_on.append(on)
        best = jnp.maximum(best, jnp.max(dots, axis=1, keepdims=True))

    stat_lane = lax.broadcasted_iota(jnp.int32, (rows, LANES), 1)
    probs = jnp.where(kept, jnp.exp(masked - best), 0.0)
    total = jnp.sum(probs, axis=1, keepdims=True)
    block_cols = jnp.zeros((rows, LANES), jnp.float32)
    for j in range(blocks_local):
        mass = jnp.sum(probs[:, j * BLKTOK : (j + 1) * BLKTOK], axis=1, keepdims=True)
        block_cols = jnp.where(lax.rem(stat_lane, blocks_local) == j, mass, block_cols)
    block_ref[...] = block_cols
    stats = jnp.where(stat_lane == 0, best, 0.0)
    unit_probs = []
    for u in range(held):
        weight = jnp.where(unit_on[u], jnp.exp(unit_masked[u] - best), 0.0)
        mass = jnp.sum(weight, axis=1, keepdims=True)
        total = total + mass
        stats = jnp.where(stat_lane == 2 + u, mass, stats)
        unit_probs.append(weight.astype(jnp.bfloat16))
    stats = jnp.where(stat_lane == 1, total, stats)

    copies[8].wait()
    accum = []
    for g in range(kv_local):
        probs_group = probs[g * group_rows : (g + 1) * group_rows]
        req_group = row_req[g * group_rows : (g + 1) * group_rows]
        accum.append(
            tree_sum(
                nn_dot(
                    jnp.where(req_group == b, probs_group, 0.0).astype(jnp.bfloat16),
                    values[b, :, g * DH : (g + 1) * DH],
                )
                for b in range(requests)
            )
        )
    accum = jnp.concatenate(accum, axis=0)
    for u in range(held):
        accum = accum + nn_dot(unit_probs[u], refill[u, 1])
    part_ref[:rows, :] = accum
    stat_rows = part_ref.shape[0] - rows
    turned = jnp.transpose(stats)
    part_ref[rows:, :] = jnp.zeros((stat_rows, LANES), jnp.float32)
    part_ref[rows:, :rows] = turned[:stat_rows]


def middle_kernel(flips, count, rows, requests, blocks_local, held, *refs):
    route_ref, block_ref, head_ref, recall_ref = refs[-4:]
    part_refs = refs[:-4]
    seq_index = lax.axis_index("seq")
    pieces = pieces_of(part_refs, count)
    stat_rows = pieces[0].shape[0] - rows
    turned = jnp.transpose(jnp.concatenate([piece[rows:] for piece in pieces], axis=0))
    stats = [turned[:rows, at * stat_rows : (at + 1) * stat_rows] for at in range(count)]
    best = functools.reduce(jnp.maximum, [stat[:, 0:1] for stat in stats])
    factors = [jnp.exp(stat[:, 0:1] - best) for stat in stats]
    total = tree_sum(stat[:, 1:2] * factor for stat, factor in zip(stats, factors))
    accum = tree_sum(piece[:rows] * factor for piece, factor in zip(pieces, factors))
    head_ref[:rows, :] = (accum / total).astype(jnp.bfloat16)

    origin = route_ref[0:1, :held]
    recall = jnp.zeros((1, held), jnp.float32)
    for at in range(count):
        share = stats[at][:, 2 : 2 + held] * factors[at] / total
        mass = jnp.sum(share, axis=0, keepdims=True)
        recall = jnp.where(origin == source_of(seq_index, flips, at), mass, recall)
    recall_ref[...] = recall

    if flips:
        own = factors[0]
    else:
        own = functools.reduce(
            lambda found, at: jnp.where(seq_index == at, factors[at], found),
            range(1, count),
            factors[0],
        )
    row = lax.broadcasted_iota(jnp.int32, (rows, LANES), 0)
    lanes = lax.broadcasted_iota(jnp.int32, (rows, LANES), 1)
    mine = lax.rem(row, requests) == lax.div(lanes, blocks_local)
    mass = jnp.sum(jnp.where(mine, block_ref[...] * own / total, 0.0), axis=0, keepdims=True)
    high = mass.astype(jnp.bfloat16).astype(jnp.float32)
    middle = (mass - high).astype(jnp.bfloat16).astype(jnp.float32)
    low = mass - high - middle
    extra = head_ref.shape[0] - rows
    line = lax.broadcasted_iota(jnp.int32, (extra, LANES), 0)
    packed = jnp.where(line == 0, high, jnp.where(line == 1, middle, 0.0))
    packed = jnp.where(line == 2, low, packed)
    head_ref[rows:, :] = packed.astype(jnp.bfloat16)


def hop_kernel(route_ref, own_ref, across_ref, out_ref):
    keep = route_ref[1:2] > 0
    for u in range(out_ref.shape[0]):
        for half in range(out_ref.shape[1]):
            out_ref[u, half] = jnp.where(keep, own_ref[u, half], across_ref[u, half])


def place_blocks(route_ref, own_ref, across_ref, beside_ref, out_ref):
    own, across = route_ref[2:3] > 0, route_ref[3:4] > 0
    for u in range(out_ref.shape[0]):
        for half in range(out_ref.shape[1]):
            moved = jnp.where(across, across_ref[u, half], beside_ref[u, half])
            out_ref[u, half] = jnp.where(own, own_ref[u, half], moved)


def final_kernel(flips, count, rows, requests, routed, acc_ref, recall_in, *refs):
    piece_refs = refs[: count if flips else 1]
    refs = refs[len(piece_refs) :]
    if routed:
        out_ref, block_ref, recall_ref, kv_ref = refs[4:]
        place_blocks(*refs[:4], kv_ref)
    else:
        out_ref, block_ref, recall_ref = refs
    recall_ref[...] = recall_in[...]
    head_index = lax.axis_index("head")
    blocks_local = acc_ref.shape[1]
    pieces = pieces_of(piece_refs, count)
    for at, piece in enumerate(pieces):
        start = source_of(head_index, flips, at) * rows
        out_ref[pl.ds(pl.multiple_of(start, rows), rows), :] = piece[:rows]
    masses = []
    for piece in pieces:
        lines = piece[rows:].astype(jnp.float32)
        masses.append(lines[0:1] + lines[1:2] + lines[2:3])
    mass = tree_sum(masses)
    lanes = lax.broadcasted_iota(jnp.int32, (1, LANES), 1)
    at_req = lax.broadcasted_iota(jnp.int32, (requests, blocks_local), 0)
    at_block = lax.broadcasted_iota(jnp.int32, (requests, blocks_local), 1)
    added = acc_ref[...]
    for b in range(requests):
        for j in range(blocks_local):
            one = jnp.sum(jnp.where(lanes == b * blocks_local + j, mass, 0.0), axis=1, keepdims=True)
            added = jnp.where((at_req == b) & (at_block == j), added + one, added)
    block_ref[...] = added


def move_blocks(refill_kv, owners, seq_index, seq_count):
    held = refill_kv.shape[0]
    steps = (owners - seq_index) % seq_count
    earlier = jnp.arange(held)[:, None] > jnp.arange(held)[None, :]
    order_in = jnp.sum((owners[:, None] == owners[None, :]) & earlier, axis=1)
    slots = seq_count * CAP
    slot_of = owners * CAP + order_in
    pick = (seq_index - steps) % seq_count * CAP + order_in
    buffer = jnp.zeros((slots,) + refill_kv.shape[1:], refill_kv.dtype).at[slot_of].set(refill_kv)
    got = lax.all_to_all(
        buffer.reshape((seq_count, CAP) + refill_kv.shape[1:]),
        "seq",
        split_axis=0,
        concat_axis=0,
        tiled=True,
    )
    return got.reshape((slots,) + refill_kv.shape[1:])[pick]


def on_device(
    query,
    cache_keys,
    cache_values,
    lengths,
    heavy,
    acc_scores,
    refill_kv,
    refill_dest,
    refill_req,
    refill_head,
):
    requests, width = query.shape
    heads_local = width // DH
    rows = heads_local * requests
    held = refill_kv.shape[0]
    blocks_local = cache_keys.shape[1] // BLKTOK
    seq_count = lax.axis_size("seq")
    head_count = lax.axis_size("head")
    seq_index = lax.axis_index("seq")
    hbm = pl.BlockSpec(memory_space=pl.ANY)
    vmem = pl.BlockSpec(memory_space=pltpu.VMEM)
    stat_rows = round_up(2 + held, 8)
    scalars = (lengths, heavy, refill_req, refill_head, refill_dest.reshape(held))
    arrays = (query, cache_keys, cache_values)
    routed = held == CAP and seq_count == 1 << CAP

    if routed:
        across = flip(refill_kv, "seq", seq_count // 2)
    else:
        recalled_kv = move_blocks(refill_kv, refill_dest[:, 0], seq_index, seq_count)

    part, block_part, route, own = pl.pallas_call(
        local_kernel,
        out_shape=(
            pltpu.VMEM((rows + stat_rows, LANES), jnp.float32),
            pltpu.VMEM((rows, LANES), jnp.float32),
            pltpu.VMEM((8, LANES), jnp.int32),
            pltpu.VMEM(refill_kv.shape, refill_kv.dtype),
        ),
        in_specs=[hbm] * (len(scalars) + len(arrays) + 1),
        out_specs=(vmem,) * 4,
        scratch_shapes=[pltpu.SMEM(value.shape, value.dtype) for value in scalars]
        + [pltpu.VMEM(value.shape, value.dtype) for value in arrays]
        + [pltpu.SemaphoreType.DMA((len(scalars) + len(arrays) + 1,))],
        name="local_attention",
    )(*scalars, *arrays, refill_kv)

    parts = exchange(part, "seq")
    if routed:
        passed = pl.pallas_call(
            hop_kernel,
            out_shape=pltpu.VMEM(refill_kv.shape, refill_kv.dtype),
            in_specs=[vmem] * 3,
            out_specs=vmem,
            name="pick_hop",
        )(near(route), near(own), near(across))
        beside = flip(passed, "seq", 1)
    head_part, recall_scores = pl.pallas_call(
        functools.partial(
            middle_kernel, by_flips(seq_count), seq_count, rows, requests, blocks_local, held
        ),
        out_shape=(
            pltpu.VMEM((rows + 16, LANES), jnp.bfloat16),
            pltpu.VMEM((1, held), jnp.float32),
        ),
        in_specs=[vmem] * (len(parts) + 2),
        out_specs=(vmem, vmem),
        name="combine_seq",
    )(*(near(value) if by_flips(seq_count) else value for value in parts), near(route), near(block_part))

    head_parts = exchange(head_part, "head")
    blocks = (route, own, across, beside) if routed else ()
    outputs = (
        jax.ShapeDtypeStruct((head_count * rows, LANES), jnp.bfloat16),
        jax.ShapeDtypeStruct(acc_scores.shape, jnp.float32),
        jax.ShapeDtypeStruct((1, held), jnp.float32),
        jax.ShapeDtypeStruct(refill_kv.shape, refill_kv.dtype),
    )[: 4 if routed else 3]
    joined = pl.pallas_call(
        functools.partial(final_kernel, by_flips(head_count), head_count, rows, requests, routed),
        out_shape=outputs,
        in_specs=[vmem] * (len(head_parts) + len(blocks) + 2),
        out_specs=(vmem,) * len(outputs),
        name="join_heads",
    )(
        acc_scores,
        near(recall_scores),
        *(near(value) for value in head_parts),
        *(near(value) for value in blocks),
    )
    attn_rows, block_scores, recall_scores = joined[:3]
    if routed:
        recalled_kv = joined[3]
    attn_out = (
        attn_rows.reshape(head_count * heads_local, requests, DH)
        .transpose(1, 0, 2)
        .reshape(requests, head_count * width)
    )
    return (attn_out, block_scores, recalled_kv, recall_scores)


def solution(mesh):
    in_specs = (
        P("groups", "head"),
        P("groups", "seq", "head"),
        P("groups", "seq", "head"),
        P("groups"),
        P("groups", None),
        P("groups", "seq"),
        P(("groups", "seq", "head"), None, None, None),
        P(("groups", "seq", "head"), None),
        P(("groups", "seq", "head")),
        P(("groups", "seq", "head")),
    )
    out_specs = (
        P("groups", None),
        P("groups", "seq"),
        P(("groups", "seq", "head"), None, None, None),
        P(("groups", "seq", "head"), None),
    )

    return jax.shard_map(
        on_device, mesh=mesh, in_specs=in_specs, out_specs=out_specs, check_vma=False
    )
```

```python
import functools
import math

import jax
import jax.numpy as jnp
from jax import lax
from jax.experimental import pallas as pl
from jax.experimental.pallas import tpu as pltpu
from jax.sharding import PartitionSpec as P


DH = 128
BLKTOK = 128
RECENT = 2
CAP = 2
LANES = 128
FEW = 4

NEG_BIG = -1e30


ORDER = (5, 6, 7, 8, 9, 3, 2, 0, 4, 1)


def round_up(value, step):
    return (value + step - 1) // step * step


def modulo(value, count):
    if count & (count - 1) == 0:
        return value & (count - 1)
    return lax.rem(value + count, jnp.full_like(value, count))


def quotient(value, count):
    if count & (count - 1) == 0:
        return value >> (count.bit_length() - 1)
    return lax.div(value, jnp.full_like(value, count))


def by_shifts(count):
    return 1 < count <= FEW and count & (count - 1) == 0


def flip(value, axis, mask):
    count = lax.axis_size(axis)
    return send(value, axis, [at ^ mask for at in range(count)])


def send(value, axis, targets):
    return lax.ppermute(value, axis, list(enumerate(targets)))


def plan_of(axis, count):
    if axis == "seq":
        shifts = [count // 2] + [at for at in range(1, count) if at != count // 2]
    else:
        shifts = [count - 1] + list(range(1, count - 1))
    return [[(at + shift) % count for at in range(count)] for shift in shifts]


def sources_of(axis, count):
    if not by_shifts(count):
        return [[at] * count for at in range(count)]
    return [list(range(count))] + [
        [targets.index(at) for at in range(count)] for targets in plan_of(axis, count)
    ]


def in_pairs(sources):
    order = [0]
    for at in range(1, len(sources)):
        if all(sources[at][sources[at][me]] == me for me in range(len(sources[at]))):
            order.append(at)
    return order[:2] + [at for at in range(1, len(sources)) if at not in order[:2]]


def exchange(value, axis):
    count = lax.axis_size(axis)
    if by_shifts(count):
        plan = plan_of(axis, count)
        return (value,) + tuple(send(value, axis, targets) for targets in plan)
    return (lax.all_gather(value, axis),)


def near(value):
    return pltpu.with_memory_space_constraint(value, pltpu.VMEM)


def pieces_of(refs, count):
    if len(refs) == count:
        return [ref[...] for ref in refs]
    return [refs[0][at] for at in range(count)]


def source_of(index, sources):
    count = len(sources)
    for mask in range(count):
        if all(source == at ^ mask for at, source in enumerate(sources)):
            return index ^ mask
    found = jnp.int32(sources[0])
    for at in range(1, count):
        found = jnp.where(index == at, sources[at], found)
    return found


def tree_sum(values):
    values = list(values)
    while len(values) > 1:
        pairs = [values[at] + values[at + 1] for at in range(0, len(values) - 1, 2)]
        if len(values) % 2:
            pairs.append(values[-1])
        values = pairs
    return values[0]


def nt_dot(left, right):
    return lax.dot_general(
        left, right, (((1,), (1,)), ((), ())), preferred_element_type=jnp.float32
    )


def nn_dot(left, right):
    return lax.dot_general(
        left, right, (((1,), (0,)), ((), ())), preferred_element_type=jnp.float32
    )


def local_kernel(*refs):
    count = (len(refs) - 4) // 2
    sources, sems = refs[:count], refs[-1]
    part_ref, block_ref, route_ref = refs[count : count + 3]
    held_refs = refs[count + 3 : -1]
    copies = []
    for at in ORDER:
        copies.append(pltpu.make_async_copy(sources[at], held_refs[at], sems.at[at]))
        copies[-1].start()
    copies = dict(zip(ORDER, copies))
    refill, _, query, keys, values, lengths, heavy, req, unit_head, dest = held_refs
    for at in (5, 6, 7, 8, 9):
        copies[at].wait()
    requests, width = query.shape
    heads_local = width // DH
    seq_local = keys.shape[1]
    kv_local = keys.shape[2] // DH
    per_group = heads_local // kv_local
    held = refill.shape[0]
    blocks_local = seq_local // BLKTOK
    rows = heads_local * requests
    group_rows = per_group * requests
    score_scale = 1.0 / math.sqrt(DH)
    seq_index = lax.axis_index("seq")
    seq_count = lax.axis_size("seq")

    origin = modulo(seq_index - modulo(dest[...] - seq_index, seq_count), seq_count)
    source = origin[:, 0:1]
    wanted = modulo(source - seq_index + (seq_index ^ 1), seq_count)
    far = seq_index ^ (seq_count // 2)
    route_ref[0:1, :held] = origin
    for line, flag in enumerate((wanted == seq_index, source == seq_index, source == far)):
        value = jnp.broadcast_to(flag.astype(jnp.int32), (1, LANES))
        route_ref[line + 1 : line + 2, :] = value

    row = lax.broadcasted_iota(jnp.int32, (rows, 1), 0)
    row_req = modulo(row, requests)
    row_group = quotient(row, group_rows)
    lane = lax.broadcasted_iota(jnp.int32, (1, seq_local), 1)
    position = lane + seq_index * seq_local
    lane_block = quotient(position, BLKTOK)
    kept = None
    for b in range(requests):
        length = lengths[:, b : b + 1]
        hit = lane_block >= quotient(length - 1, BLKTOK) - (RECENT - 1)
        for t in range(heavy.shape[1]):
            hit = hit | (lane_block == heavy[b : b + 1, t : t + 1])
        kept_b = jnp.where((position < length) & hit, 1, 0)
        kept_b = jnp.broadcast_to(kept_b, (rows, seq_local))
        kept = kept_b if kept is None else jnp.where(row_req == b, kept_b, kept)
    kept = kept > 0

    copies[2].wait()
    q_wide = query[...].astype(jnp.float32)
    q_rows = jnp.concatenate(
        [q_wide[:, i * DH : (i + 1) * DH] for i in range(heads_local)], axis=0
    ).astype(jnp.bfloat16)
    copies[3].wait()
    scores = []
    for g in range(kv_local):
        q_group = q_rows[g * group_rows : (g + 1) * group_rows]
        req_group = row_req[g * group_rows : (g + 1) * group_rows]
        found = None
        for b in range(requests):
            dots = nt_dot(q_group, keys[b, :, g * DH : (g + 1) * DH])
            found = dots if found is None else jnp.where(req_group == b, dots, found)
        scores.append(found)
    scores = jnp.concatenate(scores, axis=0) * score_scale
    masked = jnp.where(kept, scores, NEG_BIG)
    best = jnp.max(masked, axis=1, keepdims=True)

    copies[0].wait()
    unit_masked, unit_on = [], []
    for u in range(held):
        on = (row_group == unit_head[:, u : u + 1]) & (row_req == req[:, u : u + 1])
        dots = nt_dot(q_rows, refill[u, 0]) * score_scale
        dots = jnp.where(on, dots, NEG_BIG)
        unit_masked.append(dots)
        unit_on.append(on)
        best = jnp.maximum(best, jnp.max(dots, axis=1, keepdims=True))

    stat_lane = lax.broadcasted_iota(jnp.int32, (rows, LANES), 1)
    probs = jnp.where(kept, jnp.exp(masked - best), 0.0)
    total = jnp.sum(probs, axis=1, keepdims=True)
    block_cols = jnp.zeros((rows, LANES), jnp.float32)
    for j in range(blocks_local):
        mass = jnp.sum(probs[:, j * BLKTOK : (j + 1) * BLKTOK], axis=1, keepdims=True)
        block_cols = jnp.where(modulo(stat_lane, blocks_local) == j, mass, block_cols)
    block_ref[...] = block_cols
    stats = jnp.where(stat_lane == 0, best, 0.0)
    unit_probs = []
    for u in range(held):
        weight = jnp.where(unit_on[u], jnp.exp(unit_masked[u] - best), 0.0)
        mass = jnp.sum(weight, axis=1, keepdims=True)
        total = total + mass
        stats = jnp.where(stat_lane == 2 + u, mass, stats)
        unit_probs.append(weight.astype(jnp.bfloat16))
    stats = jnp.where(stat_lane == 1, total, stats)

    copies[4].wait()
    copies[1].wait()
    accum = []
    for g in range(kv_local):
        probs_group = probs[g * group_rows : (g + 1) * group_rows]
        req_group = row_req[g * group_rows : (g + 1) * group_rows]
        accum.append(
            tree_sum(
                nn_dot(
                    jnp.where(req_group == b, probs_group, 0.0).astype(jnp.bfloat16),
                    values[b, :, g * DH : (g + 1) * DH],
                )
                for b in range(requests)
            )
        )
    accum = jnp.concatenate(accum, axis=0)
    for u in range(held):
        accum = accum + nn_dot(unit_probs[u], refill[u, 1])
    part_ref[:rows, :] = accum
    stat_rows = part_ref.shape[0] - rows
    turned = jnp.transpose(stats)
    part_ref[rows:, :] = jnp.zeros((stat_rows, LANES), jnp.float32)
    part_ref[rows:, :rows] = turned[:stat_rows]


def middle_kernel(shifts, count, rows, requests, blocks_local, held, *refs):
    route_ref, block_ref, head_ref, recall_ref = refs[-4:]
    part_refs = refs[:-4]
    seq_index = lax.axis_index("seq")
    pieces = pieces_of(part_refs, count)
    stat_rows = pieces[0].shape[0] - rows
    turned = jnp.transpose(jnp.concatenate([piece[rows:] for piece in pieces], axis=0))
    stats = [turned[:rows, at * stat_rows : (at + 1) * stat_rows] for at in range(count)]
    best = functools.reduce(jnp.maximum, [stat[:, 0:1] for stat in stats])
    factors = [jnp.exp(stat[:, 0:1] - best) for stat in stats]
    order = in_pairs(sources_of("seq", count)) if shifts else range(count)
    total = tree_sum(stats[at][:, 1:2] * factors[at] for at in order)
    accum = tree_sum(pieces[at][:rows] * factors[at] for at in order)
    head_ref[:rows, :] = (accum / total).astype(jnp.bfloat16)

    origin = route_ref[0:1, :held]
    recall = jnp.zeros((1, held), jnp.float32)
    for at in range(count):
        share = stats[at][:, 2 : 2 + held] * factors[at] / total
        mass = jnp.sum(share, axis=0, keepdims=True)
        recall = jnp.where(origin == source_of(seq_index, sources_of("seq", count)[at]), mass, recall)
    recall_ref[...] = recall

    if shifts:
        own = factors[0]
    else:
        own = functools.reduce(
            lambda found, at: jnp.where(seq_index == at, factors[at], found),
            range(1, count),
            factors[0],
        )
    row = lax.broadcasted_iota(jnp.int32, (rows, LANES), 0)
    lanes = lax.broadcasted_iota(jnp.int32, (rows, LANES), 1)
    mine = modulo(row, requests) == quotient(lanes, blocks_local)
    mass = jnp.sum(jnp.where(mine, block_ref[...] * own / total, 0.0), axis=0, keepdims=True)
    high = mass.astype(jnp.bfloat16).astype(jnp.float32)
    middle = (mass - high).astype(jnp.bfloat16).astype(jnp.float32)
    low = mass - high - middle
    extra = head_ref.shape[0] - rows
    line = lax.broadcasted_iota(jnp.int32, (extra, LANES), 0)
    packed = jnp.where(line == 0, high, jnp.where(line == 1, middle, 0.0))
    packed = jnp.where(line == 2, low, packed)
    head_ref[rows:, :] = packed.astype(jnp.bfloat16)


def hop_kernel(route_ref, own_ref, across_ref, out_ref):
    keep = route_ref[1:2] > 0
    for u in range(out_ref.shape[0]):
        for half in range(out_ref.shape[1]):
            out_ref[u, half] = jnp.where(keep, own_ref[u, half], across_ref[u, half])


def final_kernel(shifts, count, rows, requests, routed, acc_ref, recall_ref, *refs):
    piece_refs = refs[: count if shifts else 1]
    refs = refs[len(piece_refs) :]
    outs = 4 if routed else 3
    if routed:
        route_ref, own_ref, across_ref, beside_ref = refs[:4]
        refs = refs[4:]
    hbm_refs, sems = refs[:outs], refs[-1]
    attn, block = refs[outs : outs + 2]
    recall_copy = pltpu.make_async_copy(recall_ref, hbm_refs[2], sems.at[2])
    recall_copy.start()
    copies = [recall_copy]
    if routed:
        blocks = refs[outs + 2]
        own, across = route_ref[2:3] > 0, route_ref[3:4] > 0
        for u in range(blocks.shape[0]):
            for half in range(blocks.shape[1]):
                moved = jnp.where(across, across_ref[u, half], beside_ref[u, half])
                blocks[u, half] = jnp.where(own, own_ref[u, half], moved)
        copies.append(pltpu.make_async_copy(blocks, hbm_refs[3], sems.at[3]))
        copies[-1].start()
    head_index = lax.axis_index("head")
    blocks_local = acc_ref.shape[1]
    pieces = pieces_of(piece_refs, count)
    for at, piece in enumerate(pieces):
        start = source_of(head_index, sources_of("head", count)[at]) * rows
        attn[pl.ds(pl.multiple_of(start, rows), rows), :] = piece[:rows]
    copies.append(pltpu.make_async_copy(attn, hbm_refs[0], sems.at[0]))
    copies[-1].start()
    masses = []
    for piece in pieces:
        lines = piece[rows:].astype(jnp.float32)
        masses.append(lines[0:1] + lines[1:2] + lines[2:3])
    order = in_pairs(sources_of("head", count)) if shifts else range(count)
    mass = tree_sum(masses[at] for at in order)
    lanes = lax.broadcasted_iota(jnp.int32, (1, LANES), 1)
    at_req = lax.broadcasted_iota(jnp.int32, (requests, blocks_local), 0)
    at_block = lax.broadcasted_iota(jnp.int32, (requests, blocks_local), 1)
    added = acc_ref[...]
    for b in range(requests):
        for j in range(blocks_local):
            one = jnp.sum(jnp.where(lanes == b * blocks_local + j, mass, 0.0), axis=1, keepdims=True)
            added = jnp.where((at_req == b) & (at_block == j), added + one, added)
    block[...] = added
    copies.append(pltpu.make_async_copy(block, hbm_refs[1], sems.at[1]))
    copies[-1].start()
    for copy in copies:
        copy.wait()


def move_blocks(refill_kv, owners, seq_index, seq_count):
    held = refill_kv.shape[0]
    steps = (owners - seq_index) % seq_count
    earlier = jnp.arange(held)[:, None] > jnp.arange(held)[None, :]
    order_in = jnp.sum((owners[:, None] == owners[None, :]) & earlier, axis=1)
    slots = seq_count * CAP
    slot_of = owners * CAP + order_in
    pick = (seq_index - steps) % seq_count * CAP + order_in
    buffer = jnp.zeros((slots,) + refill_kv.shape[1:], refill_kv.dtype).at[slot_of].set(refill_kv)
    got = lax.all_to_all(
        buffer.reshape((seq_count, CAP) + refill_kv.shape[1:]),
        "seq",
        split_axis=0,
        concat_axis=0,
        tiled=True,
    )
    return got.reshape((slots,) + refill_kv.shape[1:])[pick]


def on_device(
    query,
    cache_keys,
    cache_values,
    lengths,
    heavy,
    acc_scores,
    refill_kv,
    refill_dest,
    refill_req,
    refill_head,
):
    requests, width = query.shape
    heads_local = width // DH
    rows = heads_local * requests
    held = refill_kv.shape[0]
    blocks_local = cache_keys.shape[1] // BLKTOK
    seq_count = lax.axis_size("seq")
    head_count = lax.axis_size("head")
    seq_index = lax.axis_index("seq")
    hbm = pl.BlockSpec(memory_space=pl.ANY)
    vmem = pl.BlockSpec(memory_space=pltpu.VMEM)
    stat_rows = round_up(2 + held, 8)
    row_of = lambda value: value.reshape(1, value.size)
    inputs = (
        refill_kv,
        acc_scores,
        query,
        cache_keys,
        cache_values,
        row_of(lengths),
        heavy,
        row_of(refill_req),
        row_of(refill_head),
        row_of(refill_dest),
    )
    routed = held == CAP and seq_count == 1 << CAP

    if routed:
        across = flip(refill_kv, "seq", seq_count // 2)
    else:
        recalled_kv = move_blocks(refill_kv, refill_dest[:, 0], seq_index, seq_count)

    part, block_part, route, own, acc = pl.pallas_call(
        local_kernel,
        out_shape=(
            pltpu.VMEM((rows + stat_rows, LANES), jnp.float32),
            pltpu.VMEM((rows, LANES), jnp.float32),
            pltpu.VMEM((8, LANES), jnp.int32),
            pltpu.VMEM(refill_kv.shape, refill_kv.dtype),
            pltpu.VMEM(acc_scores.shape, acc_scores.dtype),
        ),
        in_specs=[hbm] * len(inputs),
        out_specs=(vmem,) * 5,
        scratch_shapes=[pltpu.VMEM(value.shape, value.dtype) for value in inputs[2:]]
        + [pltpu.SemaphoreType.DMA((len(inputs),))],
        name="local_attention",
    )(*inputs)

    parts = exchange(part, "seq")
    if routed:
        passed = pl.pallas_call(
            hop_kernel,
            out_shape=pltpu.VMEM(refill_kv.shape, refill_kv.dtype),
            in_specs=[vmem] * 3,
            out_specs=vmem,
            name="pick_hop",
        )(near(route), near(own), near(across))
        beside = flip(passed, "seq", 1)
    head_part, recall_scores = pl.pallas_call(
        functools.partial(
            middle_kernel, by_shifts(seq_count), seq_count, rows, requests, blocks_local, held
        ),
        out_shape=(
            pltpu.VMEM((rows + 16, LANES), jnp.bfloat16),
            pltpu.VMEM((1, held), jnp.float32),
        ),
        in_specs=[vmem] * (len(parts) + 2),
        out_specs=(vmem, vmem),
        name="combine_seq",
    )(*(near(value) if by_shifts(seq_count) else value for value in parts), near(route), near(block_part))

    head_parts = exchange(head_part, "head")
    blocks = (route, own, across, beside) if routed else ()
    outputs = (
        jax.ShapeDtypeStruct((head_count * rows, LANES), jnp.bfloat16),
        jax.ShapeDtypeStruct(acc_scores.shape, jnp.float32),
        jax.ShapeDtypeStruct((1, held), jnp.float32),
        jax.ShapeDtypeStruct(refill_kv.shape, refill_kv.dtype),
    )[: 4 if routed else 3]
    joined = pl.pallas_call(
        functools.partial(final_kernel, by_shifts(head_count), head_count, rows, requests, routed),
        out_shape=outputs,
        in_specs=[vmem] * (len(head_parts) + len(blocks) + 2),
        out_specs=(hbm,) * len(outputs),
        scratch_shapes=[
            pltpu.VMEM(outputs[at].shape, outputs[at].dtype) for at in (0, 1, 3)[: len(outputs) - 1]
        ]
        + [pltpu.SemaphoreType.DMA((len(outputs),))],
        name="join_heads",
    )(
        near(acc),
        near(recall_scores),
        *(near(value) for value in head_parts),
        *(near(value) for value in blocks),
    )
    attn_rows, block_scores, recall_scores = joined[:3]
    if routed:
        recalled_kv = joined[3]
    attn_out = (
        attn_rows.reshape(head_count * heads_local, requests, DH)
        .transpose(1, 0, 2)
        .reshape(requests, head_count * width)
    )
    return (attn_out, block_scores, recalled_kv, recall_scores)


def solution(mesh):
    in_specs = (
        P("groups", "head"),
        P("groups", "seq", "head"),
        P("groups", "seq", "head"),
        P("groups"),
        P("groups", None),
        P("groups", "seq"),
        P(("groups", "seq", "head"), None, None, None),
        P(("groups", "seq", "head"), None),
        P(("groups", "seq", "head")),
        P(("groups", "seq", "head")),
    )
    out_specs = (
        P("groups", None),
        P("groups", "seq"),
        P(("groups", "seq", "head"), None, None, None),
        P(("groups", "seq", "head"), None),
    )

    return jax.shard_map(
        on_device, mesh=mesh, in_specs=in_specs, out_specs=out_specs, check_vma=False
    )
```
